32 devices in a mesh: seq: 2 (over x), tensor: 4 (over z), bucket: 4 (over y, core).
Axes of the slice: x: 2, y: 2, z: 4, core: 2. Of those that a mesh axis runs over, the one named last changes fastest.
Arguments:
- queries: bfloat16 [4, 1024, 3072], P('bucket', ('seq', 'tensor')), may hold values from -6 to 6
- keys: bfloat16 [4, 1024, 3072], P('bucket', ('seq', 'tensor')), may hold values from -6 to 6
- values: bfloat16 [4, 1024, 3072], P('bucket', ('seq', 'tensor')), may hold values from -6 to 6
- lengths: int32 [4], P('bucket'), may hold values from 256 to 1024, as said below
- out_weight: bfloat16 [3072, 3072], P(('seq', 'bucket'), 'tensor'), may hold values from -0.109375 to 0.109375
Outputs:
- projected: bfloat16 [4, 1024, 3072], P('bucket', ('seq', 'tensor'))
The draws below stay inside these ranges and needn't reach their ends.
Inputs may be any that keep to these rules, and one draw needn't show every extreme that they name: `lengths`: each bucket has 256 to 1024 live tokens, and at least one bucket has all 1024.
All inputs are finite; a program needn't handle non-finite values.
Results may differ from the reference program's by a relative error of at most 0.018.
Values may be sent and summed in bfloat16 or wider, within the bound.
No kernel may reach another device: no remote copies, remote signals or barrier semaphores. Data moves between devices by JAX's collectives and lax.ppermute only.
A program may use at most 128 MiB of HBM per device.

```python
import jax
import jax.numpy as jnp
from jax import lax

D = 3072
HEADS = 24
HS = 128
LEN = 1024
BUCKETS = 4


def draw_queries(key, part):
    drawn = jax.random.normal(jax.random.fold_in(key, 1), (BUCKETS, LEN, D), jnp.float32)
    return jnp.clip(drawn, -6.0, 6.0).astype(jnp.bfloat16)


def draw_keys(key, part):
    drawn = jax.random.normal(jax.random.fold_in(key, 2), (BUCKETS, LEN, D), jnp.float32)
    return jnp.clip(drawn, -6.0, 6.0).astype(jnp.bfloat16)


def draw_lengths(key, part):
    drawn = jax.random.randint(jax.random.fold_in(key, 3), (BUCKETS,), LEN // 4, LEN + 1)
    fullest = jax.random.randint(jax.random.fold_in(key, 4), (), 0, BUCKETS)
    return jnp.where(jnp.arange(BUCKETS) == fullest, LEN, drawn).astype(jnp.int32)


def block_levels(rng, dims, pieces, low, top_value):
    level, own = 1.0, jax.random.fold_in(rng, 6)
    for position, parts in pieces:
        steps = jnp.exp(jax.random.uniform(jax.random.fold_in(own, position), (parts,), jnp.float32, low / len(pieces), top_value / len(pieces)))
        level = level * jnp.repeat(steps, dims[position] // parts).reshape([-1 if axis == position else 1 for axis in range(len(dims))])
    return level


def gaussian(rng, extent, width, limit, cuts=(), held_as=jnp.bfloat16):
    result = jax.random.normal(rng, extent, jnp.float32) * width
    if len(cuts) > 0:
        result = block_levels(rng, extent, cuts, -0.22, 0.18) * result
    return jnp.clip(result, min=-limit, max=limit).astype(held_as)


def setup_inputs(seed: int = 0) -> dict:
    key_list = jax.random.split(jax.random.key(seed), 6)
    queries = draw_queries(jax.random.fold_in(key_list[5], 71), 0)
    keys = draw_keys(jax.random.fold_in(key_list[5], 71), 0)
    values = gaussian(key_list[2], (BUCKETS, LEN, D), 1.0, 6.0, ((0, 4), (1, 8)))
    lengths = draw_lengths(jax.random.fold_in(key_list[5], 71), 0)
    out_weight = gaussian(key_list[4], (D, D), D ** -0.5, 0.109375, ((0, 8), (1, 4)))
    return {"queries": queries, "keys": keys, "values": values, "lengths": lengths, "out_weight": out_weight}


MASKED_SCORE = -1e30


def attend_head(query_head, key_head, value_head, usable):
    scores = jnp.dot(query_head, key_head.T, preferred_element_type=jnp.float32) * (HS ** -0.5)
    scores = jnp.where(usable[None, :], scores, MASKED_SCORE)
    row_peak = jnp.max(scores, axis=-1, keepdims=True)
    exponent = jnp.where(usable[None, :], jnp.exp(scores - row_peak), 0.0)
    numerator = jnp.dot(exponent.astype(jnp.bfloat16), value_head, preferred_element_type=jnp.float32)
    return numerator / jnp.sum(exponent, axis=-1, keepdims=True)


def reference(queries, keys, values, lengths, out_weight):
    def split_heads(array):
        return array.reshape(LEN, HEADS, HS).transpose(1, 0, 2)

    def one_bucket(inputs):
        bucket_q, bucket_k, bucket_v, live_len = inputs
        positions = jnp.arange(LEN, dtype=jnp.int32)
        usable = positions < live_len

        def one_head(trio):
            return attend_head(trio[0], trio[1], trio[2], usable)

        attended = lax.map(one_head, (split_heads(bucket_q), split_heads(bucket_k), split_heads(bucket_v)))
        mixed = attended.transpose(1, 0, 2).reshape(LEN, D)
        mixed = jnp.where(usable[:, None], mixed, 0.0).astype(jnp.bfloat16)
        return jnp.dot(mixed, out_weight, preferred_element_type=jnp.float32).astype(jnp.bfloat16)

    return lax.map(one_bucket, (queries, keys, values, lengths))
```

```python
import functools
import math

import jax
import jax.numpy as jnp
from jax import lax
from jax.experimental import pallas as pl
from jax.experimental.pallas import tpu as pltpu
from jax.sharding import PartitionSpec as P

HS = 128
LOG2E = math.log2(math.e)


MASKED_SCORE = -1e30

TOKENS = P("bucket", ("seq", "tensor"), None)
IN_SPECS = (TOKENS, TOKENS, TOKENS, P("bucket"), P(("seq", "bucket"), "tensor"))
OUT_SPECS = TOKENS


def shards(queries, keys, values, lengths, out_weight):
    tok_rows = queries.shape[1]
    n_tensor = lax.axis_size("tensor")
    tensor_index = lax.axis_index("tensor")
    live_len = lengths[0]
    local_q, local_k, local_v = (
        lax.all_to_all(queries[0], "seq", split_axis=1, concat_axis=0, tiled=True),
        lax.all_to_all(keys[0], "seq", split_axis=1, concat_axis=0, tiled=True),
        lax.all_to_all(values[0], "seq", split_axis=1, concat_axis=0, tiled=True),
    )
    row_count, col_count = local_q.shape
    head_count = col_count // HS
    query_heads = local_q.reshape(row_count, head_count, HS)

    def spots(first_row, total_rows):
        index_row = first_row + jnp.arange(total_rows, dtype=jnp.int32)
        owner = index_row // row_count
        within = index_row % row_count
        return (within // tok_rows * n_tensor + owner) * tok_rows + within % tok_rows

    query_usable = spots(tensor_index * row_count, row_count) < live_len
    initial = (
        jnp.full((row_count, head_count), MASKED_SCORE, jnp.float32),
        jnp.zeros((row_count, head_count), jnp.float32),
        jnp.zeros((row_count, head_count, HS), jnp.float32),
    )
    carried = initial
    first_row = jnp.int32(0)
    key_rows = lax.all_gather(local_k, "tensor", axis=0, tiled=True)
    value_rows = lax.all_gather(local_v, "tensor", axis=0, tiled=True)
    for offset in range(key_rows.shape[0] // row_count):
        row_peak, row_sum, accumulated = carried
        key_tile = key_rows[offset * row_count : (offset + 1) * row_count].reshape(
            row_count, head_count, HS
        )
        value_tile = value_rows[offset * row_count : (offset + 1) * row_count].reshape(
            row_count, head_count, HS
        )
        key_usable = spots(first_row + offset * row_count, row_count) < live_len
        scores = jnp.einsum(
            "qhd,khd->qhk", query_heads, key_tile, preferred_element_type=jnp.float32
        ) * HS ** (-0.5)
        scores = jnp.where(key_usable[None, None, :], scores, MASKED_SCORE)
        peak_new = jnp.maximum(row_peak, jnp.max(scores, axis=-1))
        exponent = jnp.where(key_usable[None, None, :], jnp.exp(scores - peak_new[..., None]), 0.0)
        rescale = jnp.exp(row_peak - peak_new)
        accumulated = accumulated * rescale[..., None] + jnp.einsum(
            "qhk,khd->qhd",
            exponent.astype(jnp.bfloat16),
            value_tile,
            preferred_element_type=jnp.float32,
        )
        carried = (peak_new, row_sum * rescale + jnp.sum(exponent, axis=-1), accumulated)
    row_peak, row_sum, accumulated = carried
    attended = accumulated / row_sum[..., None]
    mixed = jnp.where(query_usable[:, None], attended.reshape(row_count, col_count), 0.0).astype(
        jnp.bfloat16
    )
    restored = lax.all_to_all(mixed, "seq", split_axis=0, concat_axis=1, tiled=True)
    wide_weight = lax.all_gather(out_weight, "tensor", axis=1, tiled=True)
    summed = jnp.dot(
        restored,
        lax.all_gather(wide_weight, ("seq", "bucket"), axis=0, tiled=True),
        preferred_element_type=jnp.float32,
    )
    return summed.astype(jnp.bfloat16)[None]


def pack_kernel(dest_ref, q_ref, k_ref, v_ref, *out_refs):
    width = out_refs[0].shape[-1]
    for j, out_ref in enumerate(out_refs):
        cols = pl.ds(pl.multiple_of(dest_ref[j] * width, HS), width)
        out_ref[0] = q_ref[:, cols]
        out_ref[1] = k_ref[:, cols]
        out_ref[2] = v_ref[:, cols]


def attend_kernel(pos_ref, *refs, n_seq, n_tensor):
    groups = n_seq * n_tensor
    blocks, outs = refs[:groups], refs[groups : groups + n_tensor]
    k_scr, v_scr = refs[groups + n_tensor :]
    rows, width = blocks[0].shape[1:]
    live_len = pos_ref[groups]
    for h in range(width // HS):
        for j in range(groups):
            k_scr[h, j * rows : (j + 1) * rows, :] = blocks[j][1, :, h * HS : (h + 1) * HS]
            v_scr[h, j * rows : (j + 1) * rows, :] = blocks[j][2, :, h * HS : (h + 1) * HS]
    spot = lax.broadcasted_iota(jnp.int32, (1, rows), 1)
    bias = jnp.concatenate(
        [jnp.where(pos_ref[j] + spot < live_len, 0.0, MASKED_SCORE) for j in range(groups)], axis=1
    )
    row_spot = lax.broadcasted_iota(jnp.int32, (rows, HS), 0)
    for h in range(width // HS):
        cols = slice(h * HS, (h + 1) * HS)
        for j in range(groups):
            scores = lax.dot_general(
                blocks[j][0, :, cols], k_scr[h], (((1,), (1,)), ((), ())),
                preferred_element_type=jnp.float32,
            ) + bias
            peak = jnp.max(scores, axis=-1, keepdims=True)
            expo = jnp.exp2((scores - peak) * (HS ** -0.5 * LOG2E))
            total = jnp.sum(expo, axis=-1, keepdims=True)
            mixed = jnp.dot(expo.astype(jnp.bfloat16), v_scr[h], preferred_element_type=jnp.float32)
            mixed = jnp.where(pos_ref[j] + row_spot < live_len, mixed / total, 0.0)
            outs[j % n_tensor][j // n_tensor, :, cols] = mixed.astype(jnp.bfloat16)


def project_kernel(where_ref, *refs, row_set, n_tensor, n_bucket):
    pieces, weights = refs[:n_tensor], refs[n_tensor : n_tensor + n_bucket * n_tensor]
    out_ref, o_scr = refs[n_tensor + n_bucket * n_tensor :]
    width = weights[0].shape[1]
    z, b = where_ref[0], where_ref[1]
    for dz in range(n_tensor):
        o_scr[lax.rem(z + dz, n_tensor)] = pieces[dz][row_set]
    for dz in range(n_tensor):
        acc = None
        for m in range(n_bucket):
            part = jnp.dot(
                o_scr[jnp.bitwise_xor(b, m)], weights[m * n_tensor + dz][...],
                preferred_element_type=jnp.float32,
            )
            acc = part if acc is None else acc + part
        place = pl.multiple_of(lax.rem(z - dz + n_tensor, n_tensor) * width, HS)
        out_ref[:, pl.ds(place, width)] = acc.astype(out_ref.dtype)


def vmem_call(kernel, n_in, out_shape, scratch=(), name=None):
    vmem = pl.BlockSpec(memory_space=pltpu.VMEM)
    return pl.pallas_call(
        kernel,
        in_specs=[pl.BlockSpec(memory_space=pltpu.SMEM)] + [vmem] * n_in,
        out_specs=[vmem] * len(out_shape),
        out_shape=out_shape,
        scratch_shapes=scratch,
        name=name,
    )


def head_shards(queries, keys, values, lengths, out_weight):
    n_seq, n_tensor, n_bucket = (lax.axis_size(a) for a in ("seq", "tensor", "bucket"))
    s, z, b = (lax.axis_index(a).astype(jnp.int32) for a in ("seq", "tensor", "bucket"))
    groups = n_seq * n_tensor
    rows, model = queries.shape[1:]
    width = model // groups
    bf16, f32 = jnp.bfloat16, jnp.float32
    shifts = [(ds, dz) for ds in range(n_seq) for dz in range(n_tensor)]

    dest = jnp.stack([(s + ds) % n_seq * n_tensor + (z + dz) % n_tensor for ds, dz in shifts])
    packed = vmem_call(
        pack_kernel, 3, [jax.ShapeDtypeStruct((3, rows, width), bf16)] * groups, name="pack"
    )(dest, queries[0], keys[0], values[0])

    def shifted(x, ds, dz):
        perm = [
            (i * n_tensor + t, (i + ds) % n_seq * n_tensor + (t + dz) % n_tensor)
            for i in range(n_seq)
            for t in range(n_tensor)
        ]
        return lax.ppermute(x, ("seq", "tensor"), perm)

    blocks = [packed[0]] + [shifted(packed[j], *shifts[j]) for j in range(1, groups)]

    weights = [out_weight]
    for dz in range(1, n_tensor):
        weights.append(shifted(out_weight, 0, dz))
    bit = n_bucket // 2
    held = {0: weights}
    while bit:
        swap = [(i, i ^ bit) for i in range(n_bucket)]
        held.update(
            {m ^ bit: [lax.ppermute(w, "bucket", swap) for w in held[m]] for m in list(held)}
        )
        bit //= 2
    flat_weights = [w for m in range(n_bucket) for w in held[m]]

    pos = jnp.stack(
        [((s - ds) % n_seq * n_tensor + (z - dz) % n_tensor) * rows for ds, dz in shifts]
        + [lengths[0]]
    )
    mixed = vmem_call(
        functools.partial(attend_kernel, n_seq=n_seq, n_tensor=n_tensor),
        groups,
        [jax.ShapeDtypeStruct((n_seq, rows, width), bf16)] * n_tensor,
        [pltpu.VMEM((width // HS, groups * rows, HS), bf16)] * 2,
        name="attend",
    )(pos, *blocks)
    pieces = [mixed[0]] + [shifted(mixed[dz], 0, -dz) for dz in range(1, n_tensor)]

    def project(row_set, dtype):
        return vmem_call(
            functools.partial(
                project_kernel, row_set=row_set, n_tensor=n_tensor, n_bucket=n_bucket
            ),
            n_tensor + n_tensor * n_bucket,
            [jax.ShapeDtypeStruct((rows, model), dtype)],
            [pltpu.VMEM((n_tensor, rows, width), bf16)],
            name=f"project{row_set}",
        )(jnp.stack([z, b]), *pieces, *flat_weights)[0]

    received = [
        shifted(project(ds, bf16), -ds, 0) for ds in range(1, n_seq)
    ]
    summed = project(0, f32)
    for other in received:
        summed = summed + other.astype(f32)
    return summed.astype(bf16)[None]


def solution(mesh):
    n_seq, n_tensor, n_bucket = (mesh.shape[a] for a in ("seq", "tensor", "bucket"))

    def run(queries, keys, values, lengths, out_weight):
        heads = queries.shape[2] // HS
        by_head = (
            heads % (n_seq * n_tensor) == 0
            and n_tensor == n_bucket
            and n_bucket & (n_bucket - 1) == 0
        )
        return jax.shard_map(
            head_shards if by_head else shards,
            mesh=mesh, in_specs=IN_SPECS, out_specs=OUT_SPECS, check_vma=False,
        )(queries, keys, values, lengths, out_weight)

    return run
```

```python
import functools
import math

import jax
import jax.numpy as jnp
from jax import lax
from jax.experimental import pallas as pl
from jax.experimental.pallas import tpu as pltpu
from jax.sharding import PartitionSpec as P


HS = 128
LOG2E = math.log2(math.e)


MASKED_SCORE = -1e30

TOKENS = P("bucket", ("seq", "tensor"), None)
IN_SPECS = (TOKENS, TOKENS, TOKENS, P("bucket"), P(("seq", "bucket"), "tensor"))
OUT_SPECS = TOKENS


def shards(queries, keys, values, lengths, out_weight):
    tok_rows = queries.shape[1]
    n_tensor = lax.axis_size("tensor")
    tensor_index = lax.axis_index("tensor")
    live_len = lengths[0]
    local_q, local_k, local_v = (
        lax.all_to_all(queries[0], "seq", split_axis=1, concat_axis=0, tiled=True),
        lax.all_to_all(keys[0], "seq", split_axis=1, concat_axis=0, tiled=True),
        lax.all_to_all(values[0], "seq", split_axis=1, concat_axis=0, tiled=True),
    )
    row_count, col_count = local_q.shape
    head_count = col_count // HS
    query_heads = local_q.reshape(row_count, head_count, HS)

    def spots(first_row, total_rows):
        index_row = first_row + jnp.arange(total_rows, dtype=jnp.int32)
        owner = index_row // row_count
        within = index_row % row_count
        return (within // tok_rows * n_tensor + owner) * tok_rows + within % tok_rows

    query_usable = spots(tensor_index * row_count, row_count) < live_len
    initial = (
        jnp.full((row_count, head_count), MASKED_SCORE, jnp.float32),
        jnp.zeros((row_count, head_count), jnp.float32),
        jnp.zeros((row_count, head_count, HS), jnp.float32),
    )
    carried = initial
    first_row = jnp.int32(0)
    key_rows = lax.all_gather(local_k, "tensor", axis=0, tiled=True)
    value_rows = lax.all_gather(local_v, "tensor", axis=0, tiled=True)
    for offset in range(key_rows.shape[0] // row_count):
        row_peak, row_sum, accumulated = carried
        key_tile = key_rows[offset * row_count : (offset + 1) * row_count].reshape(
            row_count, head_count, HS
        )
        value_tile = value_rows[offset * row_count : (offset + 1) * row_count].reshape(
            row_count, head_count, HS
        )
        key_usable = spots(first_row + offset * row_count, row_count) < live_len
        scores = jnp.einsum(
            "qhd,khd->qhk", query_heads, key_tile, preferred_element_type=jnp.float32
        ) * HS ** (-0.5)
        scores = jnp.where(key_usable[None, None, :], scores, MASKED_SCORE)
        peak_new = jnp.maximum(row_peak, jnp.max(scores, axis=-1))
        exponent = jnp.where(key_usable[None, None, :], jnp.exp(scores - peak_new[..., None]), 0.0)
        rescale = jnp.exp(row_peak - peak_new)
        accumulated = accumulated * rescale[..., None] + jnp.einsum(
            "qhk,khd->qhd",
            exponent.astype(jnp.bfloat16),
            value_tile,
            preferred_element_type=jnp.float32,
        )
        carried = (peak_new, row_sum * rescale + jnp.sum(exponent, axis=-1), accumulated)
    row_peak, row_sum, accumulated = carried
    attended = accumulated / row_sum[..., None]
    mixed = jnp.where(query_usable[:, None], attended.reshape(row_count, col_count), 0.0).astype(
        jnp.bfloat16
    )
    restored = lax.all_to_all(mixed, "seq", split_axis=0, concat_axis=1, tiled=True)
    wide_weight = lax.all_gather(out_weight, "tensor", axis=1, tiled=True)
    summed = jnp.dot(
        restored,
        lax.all_gather(wide_weight, ("seq", "bucket"), axis=0, tiled=True),
        preferred_element_type=jnp.float32,
    )
    return summed.astype(jnp.bfloat16)[None]


def head_chunks(width):
    heads = width // HS
    cuts = [0, heads - heads // 2 if heads > 2 else 1, heads] if heads > 1 else [0, heads]
    return [(lo * HS, hi * HS) for lo, hi in zip(cuts, cuts[1:])]


def pack_kernel(dest_ref, q_ref, k_ref, v_ref, *out_refs, groups):
    width = q_ref.shape[1] // groups
    for c, (lo, hi) in enumerate(head_chunks(width)):
        for j in range(groups):
            out_ref = out_refs[c * groups + j]
            cols = pl.ds(pl.multiple_of(dest_ref[j] * width + lo, HS), hi - lo)
            out_ref[0] = q_ref[:, cols]
            out_ref[1] = k_ref[:, cols]
            out_ref[2] = v_ref[:, cols]


def attend_kernel(pos_ref, *refs, n_seq, n_tensor):
    groups = n_seq * n_tensor
    blocks, outs = refs[:groups], refs[groups : groups + n_tensor]
    k_scr, v_scr = refs[groups + n_tensor :]
    rows, width = blocks[0].shape[1:]
    live_len = pos_ref[groups]
    for h in range(width // HS):
        for j in range(groups):
            k_scr[h, j * rows : (j + 1) * rows, :] = blocks[j][1, :, h * HS : (h + 1) * HS]
            v_scr[h, j * rows : (j + 1) * rows, :] = blocks[j][2, :, h * HS : (h + 1) * HS]
    spot = lax.broadcasted_iota(jnp.int32, (1, rows), 1)
    bias = jnp.concatenate(
        [jnp.where(pos_ref[j] + spot < live_len, 0.0, MASKED_SCORE) for j in range(groups)], axis=1
    )
    row_spot = lax.broadcasted_iota(jnp.int32, (rows, HS), 0)
    for h in range(width // HS):
        cols = slice(h * HS, (h + 1) * HS)
        for j in range(groups):
            scores = lax.dot_general(
                blocks[j][0, :, cols], k_scr[h], (((1,), (1,)), ((), ())),
                preferred_element_type=jnp.float32,
            ) + bias
            peak = jnp.max(scores, axis=-1, keepdims=True)
            expo = jnp.exp2((scores - peak) * (HS ** -0.5 * LOG2E))
            total = jnp.sum(expo, axis=-1, keepdims=True)
            mixed = jnp.dot(expo.astype(jnp.bfloat16), v_scr[h], preferred_element_type=jnp.float32)
            mixed = jnp.where(pos_ref[j] + row_spot < live_len, mixed / total, 0.0)
            outs[j % n_tensor][j // n_tensor, :, cols] = mixed.astype(jnp.bfloat16)


def project_kernel(where_ref, *refs, row_set, n_tensor, n_bucket):
    *ins, out_ref, o_scr = refs
    pieces, weights = ins[: -n_bucket * n_tensor], ins[-n_bucket * n_tensor :]
    width = weights[0].shape[1]
    z, b = where_ref[0], where_ref[1]
    for c, (lo, hi) in enumerate(head_chunks(o_scr.shape[-1])):
        for dz in range(n_tensor):
            o_scr[lax.rem(z + dz, n_tensor), :, lo:hi] = pieces[c * n_tensor + dz][row_set]
    for dz in range(n_tensor):
        acc = None
        for m in range(n_bucket):
            part = jnp.dot(
                o_scr[jnp.bitwise_xor(b, m)], weights[m * n_tensor + dz][...],
                preferred_element_type=jnp.float32,
            )
            acc = part if acc is None else acc + part
        place = pl.multiple_of(jnp.bitwise_xor(z, dz) * width, HS)
        out_ref[:, pl.ds(place, width)] = acc.astype(out_ref.dtype)


def vmem_call(kernel, n_in, out_shape, scratch=()):
    vmem = pl.BlockSpec(memory_space=pltpu.VMEM)
    return pl.pallas_call(
        kernel,
        in_specs=[pl.BlockSpec(memory_space=pltpu.SMEM)] + [vmem] * n_in,
        out_specs=[vmem] * len(out_shape),
        out_shape=out_shape,
        scratch_shapes=scratch,
    )


def head_shards(*args):
    return head_step(*args)


def head_step(queries, keys, values, lengths, out_weight):
    n_seq, n_tensor, n_bucket = (lax.axis_size(a) for a in ("seq", "tensor", "bucket"))
    s, z, b = (lax.axis_index(a).astype(jnp.int32) for a in ("seq", "tensor", "bucket"))
    groups = n_seq * n_tensor
    rows, model = queries.shape[1:]
    width = model // groups
    bf16, f32 = jnp.bfloat16, jnp.float32
    shifts = [(ds, dz) for ds in range(n_seq) for dz in range(n_tensor)]

    dest = jnp.stack([(s + ds) % n_seq * n_tensor + (z + dz) % n_tensor for ds, dz in shifts])
    chunks = head_chunks(width)
    packed = vmem_call(
        functools.partial(pack_kernel, groups=groups),
        3,
        [jax.ShapeDtypeStruct((3, rows, hi - lo), bf16) for lo, hi in chunks for _ in range(groups)],
    )(dest, queries[0], keys[0], values[0])

    def shifted(x, ds, dz):
        perm = [
            (i * n_tensor + t, (i + ds) % n_seq * n_tensor + (t + dz) % n_tensor)
            for i in range(n_seq)
            for t in range(n_tensor)
        ]
        return lax.ppermute(x, ("seq", "tensor"), perm)

    blocks = [
        [packed[c * groups]]
        + [shifted(packed[c * groups + j], *shifts[j]) for j in range(1, groups)]
        for c in range(len(chunks))
    ]

    weights = {0: out_weight}
    bit = n_tensor // 2
    while bit:
        swap = [(i, i ^ bit) for i in range(n_tensor)]
        for e in list(weights):
            weights[e ^ bit] = lax.ppermute(weights[e], "tensor", swap)
        bit //= 2
    weights = [weights[e] for e in range(n_tensor)]
    bit = n_bucket // 2
    held = {0: weights}
    while bit:
        swap = [(i, i ^ bit) for i in range(n_bucket)]
        for m in list(held):
            held[m ^ bit] = []
            for w in held[m]:
                held[m ^ bit].append(lax.ppermute(w, "bucket", swap))
        bit //= 2
    flat_weights = [w for m in range(n_bucket) for w in held[m]]

    pos = jnp.stack(
        [((s - ds) % n_seq * n_tensor + (z - dz) % n_tensor) * rows for ds, dz in shifts]
        + [lengths[0]]
    )
    pieces = []
    for c, (lo, hi) in enumerate(chunks):
        mixed = vmem_call(
            functools.partial(attend_kernel, n_seq=n_seq, n_tensor=n_tensor),
            groups,
            [jax.ShapeDtypeStruct((n_seq, rows, hi - lo), bf16)] * n_tensor,
            [pltpu.VMEM(((hi - lo) // HS, groups * rows, HS), bf16)] * 2,
        )(pos, *blocks[c])
        pieces.append(mixed[0])
        pieces += [shifted(mixed[dz], 0, -dz) for dz in range(1, n_tensor)]

    def project(row_set, dtype):
        return vmem_call(
            functools.partial(
                project_kernel, row_set=row_set, n_tensor=n_tensor, n_bucket=n_bucket
            ),
            len(pieces) + n_tensor * n_bucket,
            [jax.ShapeDtypeStruct((rows, model), dtype)],
            [pltpu.VMEM((n_tensor, rows, width), bf16)],
        )(jnp.stack([z, b]), *pieces, *flat_weights)[0]

    received = [shifted(project(ds, bf16), -ds, 0) for ds in range(1, n_seq)]
    summed = project(0, f32)
    for other in received:
        summed = summed + other.astype(f32)
    return summed.astype(bf16)[None]


def solution(mesh):
    n_seq, n_tensor, n_bucket = (mesh.shape[a] for a in ("seq", "tensor", "bucket"))

    def run(queries, keys, values, lengths, out_weight):
        heads = queries.shape[2] // HS
        by_head = (
            heads % (n_seq * n_tensor) == 0
            and n_tensor == n_bucket
            and 1 < n_bucket
            and n_bucket & (n_bucket - 1) == 0
        )
        step = jax.shard_map(
            head_shards if by_head else shards,
            mesh=mesh, in_specs=IN_SPECS, out_specs=OUT_SPECS, check_vma=False,
        )
        return step(queries, keys, values, lengths, out_weight)

    return run
```

```python
import functools
import math

import jax
import jax.numpy as jnp
from jax import lax
from jax.experimental import pallas as pl
from jax.experimental.pallas import tpu as pltpu
from jax.sharding import PartitionSpec as P


HS = 128
LOG2E = math.log2(math.e)


MASKED_SCORE = -1e30

TOKENS = P("bucket", ("seq", "tensor"), None)
IN_SPECS = (TOKENS, TOKENS, TOKENS, P("bucket"), P(("seq", "bucket"), "tensor"))
OUT_SPECS = TOKENS


def shards(queries, keys, values, lengths, out_weight):
    tok_rows = queries.shape[1]
    n_tensor = lax.axis_size("tensor")
    tensor_index = lax.axis_index("tensor")
    live_len = lengths[0]
    local_q, local_k, local_v = (
        lax.all_to_all(queries[0], "seq", split_axis=1, concat_axis=0, tiled=True),
        lax.all_to_all(keys[0], "seq", split_axis=1, concat_axis=0, tiled=True),
        lax.all_to_all(values[0], "seq", split_axis=1, concat_axis=0, tiled=True),
    )
    row_count, col_count = local_q.shape
    head_count = col_count // HS
    query_heads = local_q.reshape(row_count, head_count, HS)

    def spots(first_row, total_rows):
        index_row = first_row + jnp.arange(total_rows, dtype=jnp.int32)
        owner = index_row // row_count
        within = index_row % row_count
        return (within // tok_rows * n_tensor + owner) * tok_rows + within % tok_rows

    query_usable = spots(tensor_index * row_count, row_count) < live_len
    initial = (
        jnp.full((row_count, head_count), MASKED_SCORE, jnp.float32),
        jnp.zeros((row_count, head_count), jnp.float32),
        jnp.zeros((row_count, head_count, HS), jnp.float32),
    )
    carried = initial
    first_row = jnp.int32(0)
    key_rows = lax.all_gather(local_k, "tensor", axis=0, tiled=True)
    value_rows = lax.all_gather(local_v, "tensor", axis=0, tiled=True)
    for offset in range(key_rows.shape[0] // row_count):
        row_peak, row_sum, accumulated = carried
        key_tile = key_rows[offset * row_count : (offset + 1) * row_count].reshape(
            row_count, head_count, HS
        )
        value_tile = value_rows[offset * row_count : (offset + 1) * row_count].reshape(
            row_count, head_count, HS
        )
        key_usable = spots(first_row + offset * row_count, row_count) < live_len
        scores = jnp.einsum(
            "qhd,khd->qhk", query_heads, key_tile, preferred_element_type=jnp.float32
        ) * HS ** (-0.5)
        scores = jnp.where(key_usable[None, None, :], scores, MASKED_SCORE)
        peak_new = jnp.maximum(row_peak, jnp.max(scores, axis=-1))
        exponent = jnp.where(key_usable[None, None, :], jnp.exp(scores - peak_new[..., None]), 0.0)
        rescale = jnp.exp(row_peak - peak_new)
        accumulated = accumulated * rescale[..., None] + jnp.einsum(
            "qhk,khd->qhd",
            exponent.astype(jnp.bfloat16),
            value_tile,
            preferred_element_type=jnp.float32,
        )
        carried = (peak_new, row_sum * rescale + jnp.sum(exponent, axis=-1), accumulated)
    row_peak, row_sum, accumulated = carried
    attended = accumulated / row_sum[..., None]
    mixed = jnp.where(query_usable[:, None], attended.reshape(row_count, col_count), 0.0).astype(
        jnp.bfloat16
    )
    restored = lax.all_to_all(mixed, "seq", split_axis=0, concat_axis=1, tiled=True)
    wide_weight = lax.all_gather(out_weight, "tensor", axis=1, tiled=True)
    summed = jnp.dot(
        restored,
        lax.all_gather(wide_weight, ("seq", "bucket"), axis=0, tiled=True),
        preferred_element_type=jnp.float32,
    )
    return summed.astype(jnp.bfloat16)[None]


def head_chunks(width):
    heads = width // HS
    cuts = [0, heads - heads // 2 if heads > 2 else 1, heads] if heads > 1 else [0, heads]
    return [(lo * HS, hi * HS) for lo, hi in zip(cuts, cuts[1:])]


def pack_kernel(dest_ref, q_ref, k_ref, v_ref, *out_refs, groups):
    width = q_ref.shape[1] // groups
    for c, (lo, hi) in enumerate(head_chunks(width)):
        for j in range(groups):
            out_ref = out_refs[c * groups + j]
            cols = pl.ds(pl.multiple_of(dest_ref[j] * width + lo, HS), hi - lo)
            out_ref[0] = q_ref[:, cols]
            out_ref[1] = k_ref[:, cols]
            out_ref[2] = v_ref[:, cols]


def attend_kernel(pos_ref, *refs, n_seq, n_tensor):
    groups = n_seq * n_tensor
    blocks, outs = refs[:groups], refs[groups : groups + n_tensor]
    k_scr, v_scr = refs[groups + n_tensor :]
    rows, width = blocks[0].shape[1:]
    live_len = pos_ref[groups]
    for h in range(width // HS):
        for j in range(groups):
            k_scr[h, j * rows : (j + 1) * rows, :] = blocks[j][1, :, h * HS : (h + 1) * HS]
            v_scr[h, j * rows : (j + 1) * rows, :] = blocks[j][2, :, h * HS : (h + 1) * HS]
    spot = lax.broadcasted_iota(jnp.int32, (1, rows), 1)
    bias = jnp.concatenate(
        [jnp.where(pos_ref[j] + spot < live_len, 0.0, MASKED_SCORE) for j in range(groups)], axis=1
    )
    row_spot = lax.broadcasted_iota(jnp.int32, (rows, HS), 0)
    for h in range(width // HS):
        cols = slice(h * HS, (h + 1) * HS)
        for j in range(groups):
            scores = lax.dot_general(
                blocks[j][0, :, cols], k_scr[h], (((1,), (1,)), ((), ())),
                preferred_element_type=jnp.float32,
            ) + bias
            peak = jnp.max(scores, axis=-1, keepdims=True)
            expo = jnp.exp2((scores - peak) * (HS ** -0.5 * LOG2E))
            total = jnp.sum(expo, axis=-1, keepdims=True)
            mixed = jnp.dot(expo.astype(jnp.bfloat16), v_scr[h], preferred_element_type=jnp.float32)
            mixed = jnp.where(pos_ref[j] + row_spot < live_len, mixed / total, 0.0)
            outs[j % n_tensor][j // n_tensor, :, cols] = mixed.astype(jnp.bfloat16)


def project_kernel(where_ref, *refs, row_set, n_tensor, n_bucket, parts):
    *ins, out_ref, o_scr = refs
    n_weights = n_bucket * len(parts)
    pieces, weights = ins[:-n_weights], ins[-n_weights:]
    width = weights[0].shape[1]
    z, b = where_ref[0], where_ref[1]
    for c, (lo, hi) in enumerate(head_chunks(o_scr.shape[-1])):
        for dz in range(n_tensor):
            o_scr[lax.rem(z + dz, n_tensor), :, lo:hi] = pieces[c * n_tensor + dz][row_set]
    for i, e in enumerate(parts):
        acc = None
        for m in range(n_bucket):
            part = jnp.dot(
                o_scr[jnp.bitwise_xor(b, m)], weights[i * n_bucket + m][...],
                preferred_element_type=jnp.float32,
            )
            acc = part if acc is None else acc + part
        slot = jnp.bitwise_and(jnp.bitwise_xor(z, e), len(parts) - 1)
        out_ref[:, pl.ds(pl.multiple_of(slot * width, HS), width)] = acc.astype(out_ref.dtype)


def finish_kernel(where_ref, own_ref, *refs, n_tensor):
    *others, out_ref = refs
    width = others[0].shape[1]
    n_groups = own_ref.shape[1] // width
    per = n_tensor // n_groups
    for g in range(n_groups):
        first = jnp.bitwise_xor(where_ref[0], g * per)
        first = first - jnp.bitwise_and(first, per - 1)
        cols = pl.ds(pl.multiple_of(first * (width // per), HS), width)
        acc = own_ref[:, cols]
        for other in others[g::n_groups]:
            acc = acc + other[...].astype(jnp.float32)
        out_ref[:, cols] = acc.astype(out_ref.dtype)


def vmem_call(kernel, n_in, out_shape, scratch=()):
    vmem = pl.BlockSpec(memory_space=pltpu.VMEM)
    return pl.pallas_call(
        kernel,
        in_specs=[pl.BlockSpec(memory_space=pltpu.SMEM)] + [vmem] * n_in,
        out_specs=[vmem] * len(out_shape),
        out_shape=out_shape,
        scratch_shapes=scratch,
    )


def head_shards(*args):
    return head_step(*args)


def head_step(queries, keys, values, lengths, out_weight):
    n_seq, n_tensor, n_bucket = (lax.axis_size(a) for a in ("seq", "tensor", "bucket"))
    s, z, b = (lax.axis_index(a).astype(jnp.int32) for a in ("seq", "tensor", "bucket"))
    groups = n_seq * n_tensor
    rows, model = queries.shape[1:]
    width = model // groups
    bf16, f32 = jnp.bfloat16, jnp.float32
    shifts = [(ds, dz) for ds in range(n_seq) for dz in range(n_tensor)]

    dest = jnp.stack([(s + ds) % n_seq * n_tensor + (z + dz) % n_tensor for ds, dz in shifts])
    chunks = head_chunks(width)
    packed = vmem_call(
        functools.partial(pack_kernel, groups=groups),
        3,
        [jax.ShapeDtypeStruct((3, rows, hi - lo), bf16) for lo, hi in chunks for _ in range(groups)],
    )(dest, queries[0], keys[0], values[0])

    def shifted(x, ds, dz):
        perm = [
            (i * n_tensor + t, (i + ds) % n_seq * n_tensor + (t + dz) % n_tensor)
            for i in range(n_seq)
            for t in range(n_tensor)
        ]
        return lax.ppermute(x, ("seq", "tensor"), perm)

    blocks = [
        [packed[c * groups]]
        + [shifted(packed[c * groups + j], *shifts[j]) for j in range(1, groups)]
        for c in range(len(chunks))
    ]

    weights = {0: out_weight}
    bit = n_tensor // 2
    while bit:
        swap = [(i, i ^ bit) for i in range(n_tensor)]
        for e in list(weights):
            weights[e ^ bit] = lax.ppermute(weights[e], "tensor", swap)
        bit //= 2
    weights = [weights[e] for e in range(n_tensor)]
    bit = n_bucket // 2
    held = {0: weights}
    while bit:
        swap = [(i, i ^ bit) for i in range(n_bucket)]
        for m in list(held):
            held[m ^ bit] = []
            for w in held[m]:
                held[m ^ bit].append(lax.ppermute(w, "bucket", swap))
        bit //= 2

    pos = jnp.stack(
        [((s - ds) % n_seq * n_tensor + (z - dz) % n_tensor) * rows for ds, dz in shifts]
        + [lengths[0]]
    )
    pieces = []
    for c, (lo, hi) in enumerate(chunks):
        mixed = vmem_call(
            functools.partial(attend_kernel, n_seq=n_seq, n_tensor=n_tensor),
            groups,
            [jax.ShapeDtypeStruct((n_seq, rows, hi - lo), bf16)] * n_tensor,
            [pltpu.VMEM(((hi - lo) // HS, groups * rows, HS), bf16)] * 2,
        )(pos, *blocks[c])
        pieces.append(mixed[0])
        pieces += [shifted(mixed[dz], 0, -dz) for dz in range(1, n_tensor)]

    where = jnp.stack([z, b])

    def project(row_set, dtype, parts):
        weights = [held[m][e] for e in parts for m in range(n_bucket)]
        return vmem_call(
            functools.partial(
                project_kernel, row_set=row_set, n_tensor=n_tensor, n_bucket=n_bucket, parts=parts
            ),
            len(pieces) + len(weights),
            [jax.ShapeDtypeStruct((rows, len(parts) * out_weight.shape[1]), dtype)],
            [pltpu.VMEM((n_tensor, rows, width), bf16)],
        )(where, *pieces, *weights)[0]

    per = n_tensor // 2
    received = [
        shifted(
            project(ds, bf16, tuple(range(g * per, (g + 1) * per))),
            -ds, 0,
        )
        for ds in range(1, n_seq)
        for g in range(2)
    ]
    own = project(0, f32, tuple(range(n_tensor)))
    return vmem_call(
        functools.partial(finish_kernel, n_tensor=n_tensor),
        1 + len(received),
        [jax.ShapeDtypeStruct((rows, own.shape[1]), bf16)],
    )(where, own, *received)[0][None]


def solution(mesh):
    n_seq, n_tensor, n_bucket = (mesh.shape[a] for a in ("seq", "tensor", "bucket"))

    def run(queries, keys, values, lengths, out_weight):
        heads = queries.shape[2] // HS
        by_head = (
            heads % (n_seq * n_tensor) == 0
            and n_tensor == n_bucket
            and 1 < n_bucket
            and 1 < n_seq
            and n_bucket & (n_bucket - 1) == 0
        )
        step = jax.shard_map(
            head_shards if by_head else shards,
            mesh=mesh, in_specs=IN_SPECS, out_specs=OUT_SPECS, check_vma=False,
        )
        return step(queries, keys, values, lengths, out_weight)

    return run
```
